32 devices in a mesh: ep: 4 (over x, core), tp: 8 (over z, y).
Axes of the slice: x: 2, y: 2, z: 4, core: 2. Of those that a mesh axis runs over, the one named last changes fastest.
Arguments:
- tokens: bfloat16 [32, 3072], P(('ep', 'tp')), may hold values from -6 to 6
- cotangent: bfloat16 [32, 3072], P(('ep', 'tp')), may hold values from -6 to 6
- routes: int32 [32, 2], P(('ep', 'tp')), may hold values from 0 to 3, as said below
- gate_weights: bfloat16 [32, 2], P(('ep', 'tp')), may hold values from 0.099609375 to 1
- w_gate: bfloat16 [4, 3072, 8192], P('ep', None, 'tp'), may hold values from -0.109375 to 0.109375
- w_up: bfloat16 [4, 3072, 8192], P('ep', None, 'tp'), may hold values from -0.109375 to 0.109375
- w_down: bfloat16 [4, 8192, 3072], P('ep', 'tp'), may hold values from -0.0625 to 0.0625
Outputs:
- layer_out: bfloat16 [32, 3072], P(('ep', 'tp'))
- grad_tokens: bfloat16 [32, 3072], P(('ep', 'tp'))
- grad_gate: bfloat16 [4, 3072, 8192], P('ep', None, 'tp')
- grad_up: bfloat16 [4, 3072, 8192], P('ep', None, 'tp')
- grad_down: bfloat16 [4, 8192, 3072], P('ep', 'tp')
The draws below stay inside these ranges and needn't reach their ends.
Inputs may be any that keep to these rules, and one draw needn't show every extreme that they name: `routes`: each token names two different experts. One expert is named by exactly 28 tokens; every other expert by at most 14 tokens, and one of them by exactly 14.
All inputs are finite; a program needn't handle non-finite values.
Results may differ from the reference program's by a relative error of at most 0.005.
Values may be sent and summed in bfloat16 or wider, within the bound.
A program may use at most 128 MiB of HBM per device.

```python
import jax
import jax.numpy as jnp

D = 3072
FF = 8192
EXPERTS = 4
TOKENS = 32
MOST = 28


def draw_routes(key, part):
    key_hot = jax.random.fold_in(key, 11)
    key_order = jax.random.fold_in(key, 12)
    key_others = jax.random.fold_in(key, 13)
    key_swap = jax.random.fold_in(key, 14)
    n_other = EXPERTS - 1
    hot_expert = jax.random.randint(key_hot, (), 0, EXPERTS).astype(jnp.int32)
    row_order = jax.random.permutation(key_order, TOKENS).astype(jnp.int32)
    position = jnp.zeros((TOKENS,), jnp.int32).at[row_order].set(jnp.arange(TOKENS, dtype=jnp.int32))
    other_order = jax.random.permutation(key_others, n_other).astype(jnp.int32)
    others = ((hot_expert + 1 + other_order) % EXPERTS).astype(jnp.int32)
    is_hot = position < MOST
    first = jnp.where(is_hot, hot_expert, others[0])
    second = jnp.where(is_hot, others[position % n_other], others[1 + position % (n_other - 1)])
    swapped = jax.random.randint(key_swap, (TOKENS,), 0, 2).astype(jnp.int32)
    column_a = jnp.where(swapped == 1, second, first)
    column_b = jnp.where(swapped == 1, first, second)
    return jnp.stack([column_a, column_b], axis=1).astype(jnp.int32)


def levels(stream_key, shape, cuts, low, high):
    loudness, own = 1.0, jax.random.fold_in(stream_key, 6)
    for dim, blocks in cuts:
        draws = jnp.exp(jax.random.uniform(jax.random.fold_in(own, dim), (blocks,), jnp.float32, low / len(cuts), high / len(cuts)))
        loudness = loudness * jnp.repeat(draws, shape[dim] // blocks).reshape([-1 if axis == dim else 1 for axis in range(len(shape))])
    return loudness


def centred(own_key, extent, width, reach, split=(), kind=jnp.bfloat16):
    array = jax.random.normal(own_key, extent, jnp.float32) * width
    if len(split) > 0:
        array = levels(own_key, extent, split, -0.22, 0.18) * array
    return jnp.clip(array, min=-reach, max=reach).astype(kind)


def setup_inputs(seed: int = 0) -> dict:
    keys = jax.random.split(jax.random.key(seed), 8)
    tokens = centred(keys[0], (TOKENS, D), 1.0, 6.0, ((0, 32),))
    cotangent = centred(keys[1], (TOKENS, D), 1.0, 6.0, ((0, 32),))
    routes = draw_routes(jax.random.fold_in(keys[7], 71), 0)
    gate_weights = jnp.clip(0.099609375 + 0.9003906 * jax.random.uniform(keys[3], (TOKENS, 2), jnp.float32) ** levels(keys[3], (TOKENS, 2), ((0, 32),), -0.2, 0.2), 0.099609375, 1.0).astype(jnp.bfloat16)
    w_gate = centred(keys[4], (EXPERTS, D, FF), D ** -0.5, 0.109375, ((0, 4), (2, 8)))
    w_up = centred(keys[5], (EXPERTS, D, FF), D ** -0.5, 0.109375, ((0, 4), (2, 8)))
    w_down = centred(keys[6], (EXPERTS, FF, D), FF ** -0.5, 0.0625, ((0, 4), (1, 8)))
    return dict(tokens=tokens, cotangent=cotangent, routes=routes, gate_weights=gate_weights, w_gate=w_gate, w_up=w_up, w_down=w_down)


def expert_pass(token_rows, cotan_rows, gate_column, gate_slice, up_slice, down_slice):
    gate_pre = jnp.dot(token_rows, gate_slice, preferred_element_type=jnp.float32)
    up_pre = jnp.dot(token_rows, up_slice, preferred_element_type=jnp.float32)
    sigmoid = jax.nn.sigmoid(gate_pre)
    silu_gate = gate_pre * sigmoid
    hidden = (silu_gate * up_pre * gate_column[:, None]).astype(jnp.bfloat16)
    output = jnp.dot(hidden, down_slice, preferred_element_type=jnp.float32)
    grad_hidden = jnp.dot(cotan_rows, down_slice.T, preferred_element_type=jnp.float32)
    grad_act = grad_hidden * gate_column[:, None]
    grad_gpre = (grad_act * up_pre * (sigmoid * (1.0 + gate_pre * (1.0 - sigmoid)))).astype(jnp.bfloat16)
    grad_upre = (grad_act * silu_gate).astype(jnp.bfloat16)
    grad_rows = jnp.dot(grad_gpre, gate_slice.T, preferred_element_type=jnp.float32) + jnp.dot(grad_upre, up_slice.T, preferred_element_type=jnp.float32)
    grad_gslice = jnp.dot(token_rows.T, grad_gpre, preferred_element_type=jnp.float32).astype(jnp.bfloat16)
    grad_uslice = jnp.dot(token_rows.T, grad_upre, preferred_element_type=jnp.float32).astype(jnp.bfloat16)
    grad_dslice = jnp.dot(hidden.T, cotan_rows, preferred_element_type=jnp.float32).astype(jnp.bfloat16)
    return output, grad_rows, grad_gslice, grad_uslice, grad_dslice


def reference(tokens, cotangent, routes, gate_weights, w_gate, w_up, w_down):
    expert_ids = jnp.arange(EXPERTS, dtype=jnp.int32)
    chosen = (routes[:, :, None] == expert_ids[None, None, :]).astype(jnp.float32)
    gate_table = jnp.sum(gate_weights.astype(jnp.float32)[:, :, None] * chosen, axis=1)
    total_out = jnp.zeros((TOKENS, D), jnp.float32)
    total_grad = jnp.zeros((TOKENS, D), jnp.float32)
    gate_grads = []
    up_grads = []
    down_grads = []
    for expert in range(EXPERTS):
        output, grad_rows, grad_gslice, grad_uslice, grad_dslice = expert_pass(tokens, cotangent, gate_table[:, expert], w_gate[expert], w_up[expert], w_down[expert])
        total_out = total_out + output
        total_grad = total_grad + grad_rows
        gate_grads.append(grad_gslice)
        up_grads.append(grad_uslice)
        down_grads.append(grad_dslice)
    return (total_out.astype(jnp.bfloat16), total_grad.astype(jnp.bfloat16), jnp.stack(gate_grads), jnp.stack(up_grads), jnp.stack(down_grads))
```

```python
import functools

import jax
import jax.numpy as jnp
from jax import lax
from jax.experimental import pallas as pl
from jax.experimental.pallas import tpu as pltpu
from jax.sharding import PartitionSpec as P

LANES = 128
PIECE = 16
MESH = pl.DeviceIdType.MESH


def up_to(value, step):
    return -(-value // step) * step


def dot_nn(left, right):
    return lax.dot_general(left, right, (((1,), (0,)), ((), ())), preferred_element_type=jnp.float32)


def dot_nt(left, right):
    return lax.dot_general(left, right, (((1,), (1,)), ((), ())), preferred_element_type=jnp.float32)


def dot_tn(left, right):
    return lax.dot_general(left, right, (((0,), (0,)), ((), ())), preferred_element_type=jnp.float32)


def expert_kernel(
    n_ep, n_tp, own, pad,
    tokens_ref, cotan_ref, routes_ref, gates_ref, wg_hbm, wu_hbm, wd_hbm,
    tok, cot, hid, ggp, gup, res,
    row32, gath, flat, wg, wu, wd, snd32, snd, pair, half, rcv,
    w_sem, ag_send, ag_recv, fw_send, fw_recv, pr_send, pr_recv, rs_send, rs_recv,
):
    ep, tp = lax.axis_index("ep"), lax.axis_index("tp")
    side, col = lax.rem(ep, 2), ep // 2
    n_half = n_ep * n_tp // 2
    mine = col * n_tp + tp
    partner = (2 * col + 1 - side, tp)
    total, model = tok.shape
    groups = model // LANES
    n_chunks, _, width = wg.shape
    n_pieces = snd.shape[0]

    def peer(step):
        other = lax.rem(mine + step, n_half)
        return (2 * (other // n_tp) + side, lax.rem(other, n_tp))

    barrier = pltpu.get_barrier_semaphore()
    pl.semaphore_signal(barrier, inc=1, device_id=partner, device_id_type=MESH)

    @pl.loop(1, n_half)
    def _(step):
        pl.semaphore_signal(barrier, inc=1, device_id=peer(step), device_id_type=MESH)

    def weight_copies(c):
        columns = pl.ds(pl.multiple_of(c * width, width), width)
        return (
            pltpu.make_async_copy(wg_hbm.at[:, columns], wg.at[c], w_sem.at[0, c]),
            pltpu.make_async_copy(wu_hbm.at[:, columns], wu.at[c], w_sem.at[1, c]),
            pltpu.make_async_copy(wd_hbm.at[columns, :], wd.at[c], w_sem.at[2, c]),
        )

    for c in range(n_chunks):
        for copy in weight_copies(c):
            copy.start()

    row32[...] = jnp.zeros_like(row32)
    ids = lax.broadcasted_iota(jnp.int32, (1, LANES), 1)
    for r in range(own):
        for j in range(groups):
            lanes = slice(j * LANES, (j + 1) * LANES)
            at = r * pad + j
            row32[at:at + 1, :] = tokens_ref[r:r + 1, lanes].astype(jnp.float32)
            row32[at + groups:at + groups + 1, :] = cotan_ref[r:r + 1, lanes].astype(jnp.float32)
        gates = jnp.zeros((1, LANES), jnp.float32)
        for k in range(routes_ref.shape[1]):
            chosen = ids == routes_ref[r:r + 1, k:k + 1]
            gates = gates + jnp.where(chosen, gates_ref[r:r + 1, k:k + 1].astype(jnp.float32), 0.0)
        at = r * pad + 2 * groups
        row32[at:at + 1, :] = gates
    gath[0, 0] = row32[...].astype(jnp.bfloat16)

    pl.semaphore_wait(barrier, n_half)

    @pl.loop(1, n_half)
    def _(step):
        pltpu.make_async_remote_copy(
            src_ref=gath.at[0, 0], dst_ref=gath.at[0, step], send_sem=ag_send, recv_sem=ag_recv,
            device_id=peer(step), device_id_type=MESH,
        ).start()

    block = own * pad
    others = pl.ds(1, n_half - 1)
    pltpu.make_async_copy(gath.at[0, others], gath.at[0, others], ag_recv).wait()
    forward = pltpu.make_async_remote_copy(
        src_ref=gath.at[0], dst_ref=gath.at[1], send_sem=fw_send, recv_sem=fw_recv,
        device_id=partner, device_id_type=MESH,
    )
    forward.start()

    def spread(which, its_side):
        @pl.loop(0, n_half)
        def _(step):
            source = lax.rem(mine + n_half - step, n_half)
            device = (2 * (source // n_tp) + its_side) * n_tp + lax.rem(source, n_tp)
            flat[pl.ds(pl.multiple_of(device * block, 8), block), :] = (
                gath[which, step].astype(jnp.float32)
            )

    spread(0, side)
    forward.wait_recv()
    spread(1, 1 - side)

    for j in range(groups):
        tok[:, j * LANES:(j + 1) * LANES] = flat[pl.ds(j, total, stride=pad), :].astype(jnp.bfloat16)
        cot[:, j * LANES:(j + 1) * LANES] = flat[pl.ds(groups + j, total, stride=pad), :].astype(jnp.bfloat16)
    gate_rows = flat[pl.ds(2 * groups, total, stride=pad), :]
    lane = lax.broadcasted_iota(jnp.int32, gate_rows.shape, 1)
    gate = jnp.sum(jnp.where(lane == ep, gate_rows, 0.0), axis=1, keepdims=True)

    @pl.loop(0, n_chunks)
    def _(c):
        for copy in weight_copies(c):
            copy.wait()
        gate_pre = dot_nn(tok[...], wg[c])
        up_pre = dot_nn(tok[...], wu[c])
        grad_act = dot_nt(cot[...], wd[c]) * gate
        sigmoid = jax.nn.sigmoid(gate_pre)
        silu = gate_pre * sigmoid
        columns = pl.ds(pl.multiple_of(c * width, width), width)
        hid[:, columns] = (silu * up_pre * gate).astype(jnp.bfloat16)
        ggp[:, columns] = (
            grad_act * up_pre * (sigmoid * (1.0 + gate_pre * (1.0 - sigmoid)))
        ).astype(jnp.bfloat16)
        gup[:, columns] = (grad_act * silu).astype(jnp.bfloat16)

    def pair_copy(p):
        return pltpu.make_async_remote_copy(
            src_ref=snd.at[p, 1 - side], dst_ref=pair.at[p],
            send_sem=pr_send.at[p], recv_sem=pr_recv.at[p],
            device_id=partner, device_id_type=MESH,
        )

    def home_copies(p):
        pair_copy(p).wait_recv()
        half[p] = (
            snd[p, side].astype(jnp.float32) + pair[p].astype(jnp.float32)
        ).astype(jnp.bfloat16)

        @pl.loop(1, n_half)
        def _(step):
            pltpu.make_async_remote_copy(
                src_ref=half.at[p, lax.rem(mine + step, n_half)], dst_ref=rcv.at[p, step - 1],
                send_sem=rs_send.at[p], recv_sem=rs_recv.at[p],
                device_id=peer(step), device_id_type=MESH,
            ).start()

    unit = min(4, groups)
    for p in range(n_pieces):
        for first in range(p * PIECE, min((p + 1) * PIECE, 2 * groups), unit):
            start = (first % groups) * LANES
            cols = slice(start, start + unit * LANES)
            value = None
            for c in range(n_chunks):
                inner = slice(c * width, (c + 1) * width)
                if first < groups:
                    term = dot_nn(hid[:, inner], wd[c, :, cols])
                else:
                    term = dot_nt(ggp[:, inner], wg[c, cols, :]) + dot_nt(gup[:, inner], wu[c, cols, :])
                value = term if value is None else value + term
            for k in range(unit):
                snd32[pl.ds(first - p * PIECE + k, total, stride=PIECE), :] = (
                    value[:, k * LANES:(k + 1) * LANES]
                )
        for d in range(2 * n_half):
            d_ep, d_tp = divmod(d, n_tp)
            snd[p, d_ep % 2, (d_ep // 2) * n_tp + d_tp] = (
                snd32[d * own * PIECE:(d + 1) * own * PIECE, :].astype(jnp.bfloat16)
            )
        pair_copy(p).start()
        if p > 0:
            home_copies(p - 1)
    home_copies(n_pieces - 1)

    for p in range(n_pieces):
        pltpu.make_async_copy(rcv.at[p], rcv.at[p], rs_recv.at[p]).wait()
        res[p] = lax.fori_loop(
            0, n_half - 1, lambda s, acc: acc + rcv[p, s].astype(jnp.float32),
            half[p, mine].astype(jnp.float32),
        )
    pltpu.make_async_copy(gath.at[0, others], gath.at[0, others], ag_send).wait()
    forward.wait_send()
    for p in range(n_pieces):
        pair_copy(p).wait_send()
        pltpu.make_async_copy(rcv.at[p], rcv.at[p], rs_send.at[p]).wait()


def weight_kernel(own, tok, cot, hid, ggp, gup, res, dg_hbm, du_hbm, dd_hbm, out, dtok, dg, du, dd, sem):
    model, hidden = dg.shape
    tall = 192 if model % 192 == 0 else LANES
    wide = min(LANES, hidden)
    n_tall, n_wide = model // tall, hidden // wide
    done = 0
    for i in range(n_tall):
        rows = slice(i * tall, (i + 1) * tall)
        dg[rows, :] = dot_tn(tok[:, rows], ggp[...]).astype(jnp.bfloat16)
        pltpu.make_async_copy(dg.at[rows], dg_hbm.at[rows], sem.at[0]).start()
        du[rows, :] = dot_tn(tok[:, rows], gup[...]).astype(jnp.bfloat16)
        pltpu.make_async_copy(du.at[rows], du_hbm.at[rows], sem.at[1]).start()
        while done * n_tall < (i + 1) * n_wide:
            lines = slice(done * wide, (done + 1) * wide)
            dd[lines, :] = dot_tn(hid[:, lines], cot[...]).astype(jnp.bfloat16)
            pltpu.make_async_copy(dd.at[lines], dd_hbm.at[lines], sem.at[2]).start()
            done += 1

    groups = out.shape[1] // LANES
    for r in range(own):
        for j in range(2 * groups):
            line = res[j // PIECE, r * PIECE + j % PIECE:r * PIECE + j % PIECE + 1, :]
            k = j % groups
            ref = out if j < groups else dtok
            ref[r:r + 1, k * LANES:(k + 1) * LANES] = line.astype(jnp.bfloat16)

    pltpu.make_async_copy(dg, dg_hbm, sem.at[0]).wait()
    pltpu.make_async_copy(du, du_hbm, sem.at[1]).wait()
    pltpu.make_async_copy(dd, dd_hbm, sem.at[2]).wait()


def on_device(n_ep, n_tp, tokens, cotangent, routes, gate_weights, w_gate, w_up, w_down):
    n = n_ep * n_tp
    own, model = tokens.shape
    hidden = w_gate.shape[2]
    total = own * n
    groups = model // LANES
    used = 2 * groups + 1
    pad = up_to(used, PIECE)
    width = min(256, hidden)
    n_chunks = hidden // width
    n_pieces = up_to(2 * groups, PIECE) // PIECE

    vmem = pl.BlockSpec(memory_space=pltpu.VMEM)
    hbm = pl.BlockSpec(memory_space=pl.ANY)
    bf16 = jnp.bfloat16
    n_half = n // 2
    tok, cot, hid, ggp, gup, res = pl.pallas_call(
        functools.partial(expert_kernel, n_ep, n_tp, own, pad),
        out_shape=(
            jax.ShapeDtypeStruct((total, model), bf16),
            jax.ShapeDtypeStruct((total, model), bf16),
            jax.ShapeDtypeStruct((total, hidden), bf16),
            jax.ShapeDtypeStruct((total, hidden), bf16),
            jax.ShapeDtypeStruct((total, hidden), bf16),
            jax.ShapeDtypeStruct((n_pieces, own * PIECE, LANES), jnp.float32),
        ),
        in_specs=[vmem] * 4 + [hbm] * 3,
        out_specs=(vmem,) * 6,
        scratch_shapes=[
            pltpu.VMEM((own * pad, LANES), jnp.float32),
            pltpu.VMEM((2, n_half, own * pad, LANES), bf16),
            pltpu.VMEM((total * pad, LANES), jnp.float32),
            pltpu.VMEM((n_chunks, model, width), bf16),
            pltpu.VMEM((n_chunks, model, width), bf16),
            pltpu.VMEM((n_chunks, width, model), bf16),
            pltpu.VMEM((total * PIECE, LANES), jnp.float32),
            pltpu.VMEM((n_pieces, 2, n_half, own * PIECE, LANES), bf16),
            pltpu.VMEM((n_pieces, n_half, own * PIECE, LANES), bf16),
            pltpu.VMEM((n_pieces, n_half, own * PIECE, LANES), bf16),
            pltpu.VMEM((n_pieces, n_half - 1, own * PIECE, LANES), bf16),
            pltpu.SemaphoreType.DMA((3, n_chunks)),
            pltpu.SemaphoreType.DMA,
            pltpu.SemaphoreType.DMA,
            pltpu.SemaphoreType.DMA,
            pltpu.SemaphoreType.DMA,
            pltpu.SemaphoreType.DMA((n_pieces,)),
            pltpu.SemaphoreType.DMA((n_pieces,)),
            pltpu.SemaphoreType.DMA((n_pieces,)),
            pltpu.SemaphoreType.DMA((n_pieces,)),
        ],
        compiler_params=pltpu.CompilerParams(
            collective_id=0, has_side_effects=True, vmem_limit_bytes=56 * 2**20
        ),
        name="expert",
    )(tokens, cotangent, routes, gate_weights, w_gate[0], w_up[0], w_down[0])

    dg, du, dd, out, dtok = pl.pallas_call(
        functools.partial(weight_kernel, own),
        out_shape=(
            jax.ShapeDtypeStruct((model, hidden), bf16),
            jax.ShapeDtypeStruct((model, hidden), bf16),
            jax.ShapeDtypeStruct((hidden, model), bf16),
            jax.ShapeDtypeStruct((own, model), bf16),
            jax.ShapeDtypeStruct((own, model), bf16),
        ),
        in_specs=[vmem] * 6,
        out_specs=(hbm,) * 3 + (vmem,) * 2,
        scratch_shapes=[
            pltpu.VMEM((model, hidden), bf16),
            pltpu.VMEM((model, hidden), bf16),
            pltpu.VMEM((hidden, model), bf16),
            pltpu.SemaphoreType.DMA((3,)),
        ],
        compiler_params=pltpu.CompilerParams(vmem_limit_bytes=60 * 2**20),
        name="weights",
    )(tok, cot, hid, ggp, gup, res)

    return (out, dtok, dg[None], du[None], dd[None])


def solution(mesh):
    placed = (
        P(("ep", "tp"), None),
        P(("ep", "tp"), None),
        P(("ep", "tp"), None),
        P(("ep", "tp"), None),
        P("ep", None, "tp"),
        P("ep", None, "tp"),
        P("ep", "tp", None),
    )
    return jax.shard_map(
        functools.partial(on_device, mesh.shape["ep"], mesh.shape["tp"]),
        mesh=mesh,
        in_specs=placed,
        out_specs=(
            P(("ep", "tp"), None),
            P(("ep", "tp"), None),
            P("ep", None, "tp"),
            P("ep", None, "tp"),
            P("ep", "tp", None),
        ),
        check_vma=False,
    )
```

```python
import functools

import jax
import jax.numpy as jnp
from jax import lax
from jax.experimental import pallas as pl
from jax.experimental.pallas import tpu as pltpu
from jax.sharding import PartitionSpec as P

LANES = 128
PIECE = 16
MESH = pl.DeviceIdType.MESH


def up_to(value, step):
    return -(-value // step) * step


def dot_nn(left, right):
    return lax.dot_general(left, right, (((1,), (0,)), ((), ())), preferred_element_type=jnp.float32)


def dot_nt(left, right):
    return lax.dot_general(left, right, (((1,), (1,)), ((), ())), preferred_element_type=jnp.float32)


def dot_tn(left, right):
    return lax.dot_general(left, right, (((0,), (0,)), ((), ())), preferred_element_type=jnp.float32)


def expert_kernel(
    n_ep, n_tp, own, pad,
    tokens_ref, cotan_ref, routes_ref, gates_ref, wg_hbm, wu_hbm, wd_hbm,
    tok, cot, hid, ggp, gup, res,
    row32, gath, flat, wg, wu, wd, snd32, snd, pair, half, rcv,
    w_sem, ag_send, ag_recv, fw_send, fw_recv, pr_send, pr_recv, rs_send, rs_recv,
):
    ep, tp = lax.axis_index("ep"), lax.axis_index("tp")
    side, col = lax.rem(ep, 2), ep // 2
    n_half = n_ep * n_tp // 2
    mine = col * n_tp + tp
    partner = (2 * col + 1 - side, tp)
    total, model = tok.shape
    groups = model // LANES
    n_chunks, _, width = wg.shape
    n_pieces = snd.shape[0]

    def peer(step):
        other = lax.rem(mine + step, n_half)
        return (2 * (other // n_tp) + side, lax.rem(other, n_tp))

    barrier = pltpu.get_barrier_semaphore()
    pl.semaphore_signal(barrier, inc=1, device_id=partner, device_id_type=MESH)

    @pl.loop(1, n_half)
    def _(step):
        pl.semaphore_signal(barrier, inc=1, device_id=peer(step), device_id_type=MESH)

    def weight_copies(c):
        columns = pl.ds(pl.multiple_of(c * width, width), width)
        return (
            pltpu.make_async_copy(wg_hbm.at[:, columns], wg.at[c], w_sem.at[0, c]),
            pltpu.make_async_copy(wu_hbm.at[:, columns], wu.at[c], w_sem.at[1, c]),
            pltpu.make_async_copy(wd_hbm.at[columns, :], wd.at[c], w_sem.at[2, c]),
        )

    for c in range(n_chunks):
        for copy in weight_copies(c):
            copy.start()

    row32[...] = jnp.zeros_like(row32)
    ids = lax.broadcasted_iota(jnp.int32, (1, LANES), 1)
    for r in range(own):
        for j in range(groups):
            lanes = slice(j * LANES, (j + 1) * LANES)
            at = r * pad + j
            row32[at:at + 1, :] = tokens_ref[r:r + 1, lanes].astype(jnp.float32)
            row32[at + groups:at + groups + 1, :] = cotan_ref[r:r + 1, lanes].astype(jnp.float32)
        gates = jnp.zeros((1, LANES), jnp.float32)
        for k in range(routes_ref.shape[1]):
            chosen = ids == routes_ref[r:r + 1, k:k + 1]
            gates = gates + jnp.where(chosen, gates_ref[r:r + 1, k:k + 1].astype(jnp.float32), 0.0)
        at = r * pad + 2 * groups
        row32[at:at + 1, :] = gates
    gath[0, 0] = row32[...].astype(jnp.bfloat16)

    pl.semaphore_wait(barrier, n_half)

    n_layers = 1
    while n_layers * n_layers < n_tp:
        n_layers *= 2
    per = n_tp // n_layers
    spots = n_half // n_layers
    low = tp // per < n_layers // 2

    @pl.loop(0, n_half)
    def _(turn):
        its_layer = jnp.where(low, n_layers - 1 - turn // spots, turn // spots)
        its_spot = lax.rem(mine + turn, spots)
        other = (its_spot // per) * n_tp + its_layer * per + lax.rem(its_spot, per)
        step = lax.rem(other - mine + n_half, n_half)

        @pl.when(step != 0)
        def _():
            pltpu.make_async_remote_copy(
                src_ref=gath.at[0, 0], dst_ref=gath.at[0, step], send_sem=ag_send, recv_sem=ag_recv,
                device_id=peer(step), device_id_type=MESH,
            ).start()

    block = own * pad
    others = pl.ds(1, n_half - 1)
    pltpu.make_async_copy(gath.at[0, others], gath.at[0, others], ag_recv).wait()
    forward = pltpu.make_async_remote_copy(
        src_ref=gath.at[0], dst_ref=gath.at[1], send_sem=fw_send, recv_sem=fw_recv,
        device_id=partner, device_id_type=MESH,
    )
    forward.start()

    def spread(which, its_side):
        @pl.loop(0, n_half)
        def _(step):
            source = lax.rem(mine + n_half - step, n_half)
            device = (2 * (source // n_tp) + its_side) * n_tp + lax.rem(source, n_tp)
            flat[pl.ds(pl.multiple_of(device * block, 8), block), :] = (
                gath[which, step].astype(jnp.float32)
            )

    spread(0, side)
    forward.wait_recv()
    spread(1, 1 - side)

    for j in range(groups):
        tok[:, j * LANES:(j + 1) * LANES] = flat[pl.ds(j, total, stride=pad), :].astype(jnp.bfloat16)
        cot[:, j * LANES:(j + 1) * LANES] = flat[pl.ds(groups + j, total, stride=pad), :].astype(jnp.bfloat16)
    gate_rows = flat[pl.ds(2 * groups, total, stride=pad), :]
    lane = lax.broadcasted_iota(jnp.int32, gate_rows.shape, 1)
    gate = jnp.sum(jnp.where(lane == ep, gate_rows, 0.0), axis=1, keepdims=True)

    @pl.loop(0, n_chunks)
    def _(c):
        for copy in weight_copies(c):
            copy.wait()
        gate_pre = dot_nn(tok[...], wg[c])
        up_pre = dot_nn(tok[...], wu[c])
        grad_act = dot_nt(cot[...], wd[c]) * gate
        sigmoid = jax.nn.sigmoid(gate_pre)
        silu = gate_pre * sigmoid
        columns = pl.ds(pl.multiple_of(c * width, width), width)
        hid[:, columns] = (silu * up_pre * gate).astype(jnp.bfloat16)
        ggp[:, columns] = (
            grad_act * up_pre * (sigmoid * (1.0 + gate_pre * (1.0 - sigmoid)))
        ).astype(jnp.bfloat16)
        gup[:, columns] = (grad_act * silu).astype(jnp.bfloat16)

    def pair_copy(p):
        return pltpu.make_async_remote_copy(
            src_ref=snd.at[p, 1 - side], dst_ref=pair.at[p],
            send_sem=pr_send.at[p], recv_sem=pr_recv.at[p],
            device_id=partner, device_id_type=MESH,
        )

    def home_copies(p):
        pair_copy(p).wait_recv()
        half[p] = (
            snd[p, side].astype(jnp.float32) + pair[p].astype(jnp.float32)
        ).astype(jnp.bfloat16)

        @pl.loop(1, n_half)
        def _(step):
            pltpu.make_async_remote_copy(
                src_ref=half.at[p, lax.rem(mine + step, n_half)], dst_ref=rcv.at[p, step - 1],
                send_sem=rs_send.at[p], recv_sem=rs_recv.at[p],
                device_id=peer(step), device_id_type=MESH,
            ).start()

    unit = min(4, groups)
    for p in range(n_pieces):
        for first in range(p * PIECE, min((p + 1) * PIECE, 2 * groups), unit):
            start = (first % groups) * LANES
            cols = slice(start, start + unit * LANES)
            value = None
            for c in range(n_chunks):
                inner = slice(c * width, (c + 1) * width)
                if first < groups:
                    term = dot_nn(hid[:, inner], wd[c, :, cols])
                else:
                    term = dot_nt(ggp[:, inner], wg[c, cols, :]) + dot_nt(gup[:, inner], wu[c, cols, :])
                value = term if value is None else value + term
            for k in range(unit):
                snd32[pl.ds(first - p * PIECE + k, total, stride=PIECE), :] = (
                    value[:, k * LANES:(k + 1) * LANES]
                )
        for d in range(2 * n_half):
            d_ep, d_tp = divmod(d, n_tp)
            snd[p, d_ep % 2, (d_ep // 2) * n_tp + d_tp] = (
                snd32[d * own * PIECE:(d + 1) * own * PIECE, :].astype(jnp.bfloat16)
            )
        pair_copy(p).start()
        if p > 0:
            home_copies(p - 1)
    home_copies(n_pieces - 1)

    for p in range(n_pieces):
        pltpu.make_async_copy(rcv.at[p], rcv.at[p], rs_recv.at[p]).wait()
        res[p] = lax.fori_loop(
            0, n_half - 1, lambda s, acc: acc + rcv[p, s].astype(jnp.float32),
            half[p, mine].astype(jnp.float32),
        )
    pltpu.make_async_copy(gath.at[0, others], gath.at[0, others], ag_send).wait()
    forward.wait_send()
    for p in range(n_pieces):
        pair_copy(p).wait_send()
        pltpu.make_async_copy(rcv.at[p], rcv.at[p], rs_send.at[p]).wait()


def weight_kernel(own, tok, cot, hid, ggp, gup, res, dg_hbm, du_hbm, dd_hbm, out, dtok, dg, du, dd, sem):
    model, hidden = dg.shape
    tall = 192 if model % 192 == 0 else LANES
    wide = min(LANES, hidden)
    n_tall, n_wide = model // tall, hidden // wide
    done = 0
    for i in range(n_tall):
        rows = slice(i * tall, (i + 1) * tall)
        dg[rows, :] = dot_tn(tok[:, rows], ggp[...]).astype(jnp.bfloat16)
        pltpu.make_async_copy(dg.at[rows], dg_hbm.at[rows], sem.at[0]).start()
        du[rows, :] = dot_tn(tok[:, rows], gup[...]).astype(jnp.bfloat16)
        pltpu.make_async_copy(du.at[rows], du_hbm.at[rows], sem.at[1]).start()
        while done * n_tall < (i + 1) * n_wide:
            lines = slice(done * wide, (done + 1) * wide)
            dd[lines, :] = dot_tn(hid[:, lines], cot[...]).astype(jnp.bfloat16)
            pltpu.make_async_copy(dd.at[lines], dd_hbm.at[lines], sem.at[2]).start()
            done += 1

    groups = out.shape[1] // LANES
    for r in range(own):
        for j in range(2 * groups):
            line = res[j // PIECE, r * PIECE + j % PIECE:r * PIECE + j % PIECE + 1, :]
            k = j % groups
            ref = out if j < groups else dtok
            ref[r:r + 1, k * LANES:(k + 1) * LANES] = line.astype(jnp.bfloat16)

    pltpu.make_async_copy(dg, dg_hbm, sem.at[0]).wait()
    pltpu.make_async_copy(du, du_hbm, sem.at[1]).wait()
    pltpu.make_async_copy(dd, dd_hbm, sem.at[2]).wait()


def on_device(n_ep, n_tp, tokens, cotangent, routes, gate_weights, w_gate, w_up, w_down):
    n = n_ep * n_tp
    own, model = tokens.shape
    hidden = w_gate.shape[2]
    total = own * n
    groups = model // LANES
    used = 2 * groups + 1
    pad = up_to(used, 8)
    width = min(256, hidden)
    n_chunks = hidden // width
    n_pieces = up_to(2 * groups, PIECE) // PIECE

    vmem = pl.BlockSpec(memory_space=pltpu.VMEM)
    hbm = pl.BlockSpec(memory_space=pl.ANY)
    bf16 = jnp.bfloat16
    n_half = n // 2
    tok, cot, hid, ggp, gup, res = pl.pallas_call(
        functools.partial(expert_kernel, n_ep, n_tp, own, pad),
        out_shape=(
            pltpu.VMEM((total, model), bf16),
            pltpu.VMEM((total, model), bf16),
            pltpu.VMEM((total, hidden), bf16),
            pltpu.VMEM((total, hidden), bf16),
            pltpu.VMEM((total, hidden), bf16),
            pltpu.VMEM((n_pieces, own * PIECE, LANES), jnp.float32),
        ),
        in_specs=[vmem] * 4 + [hbm] * 3,
        out_specs=(vmem,) * 6,
        scratch_shapes=[
            pltpu.VMEM((own * pad, LANES), jnp.float32),
            pltpu.VMEM((2, n_half, own * pad, LANES), bf16),
            pltpu.VMEM((total * pad, LANES), jnp.float32),
            pltpu.VMEM((n_chunks, model, width), bf16),
            pltpu.VMEM((n_chunks, model, width), bf16),
            pltpu.VMEM((n_chunks, width, model), bf16),
            pltpu.VMEM((total * PIECE, LANES), jnp.float32),
            pltpu.VMEM((n_pieces, 2, n_half, own * PIECE, LANES), bf16),
            pltpu.VMEM((n_pieces, n_half, own * PIECE, LANES), bf16),
            pltpu.VMEM((n_pieces, n_half, own * PIECE, LANES), bf16),
            pltpu.VMEM((n_pieces, n_half - 1, own * PIECE, LANES), bf16),
            pltpu.SemaphoreType.DMA((3, n_chunks)),
            pltpu.SemaphoreType.DMA,
            pltpu.SemaphoreType.DMA,
            pltpu.SemaphoreType.DMA,
            pltpu.SemaphoreType.DMA,
            pltpu.SemaphoreType.DMA((n_pieces,)),
            pltpu.SemaphoreType.DMA((n_pieces,)),
            pltpu.SemaphoreType.DMA((n_pieces,)),
            pltpu.SemaphoreType.DMA((n_pieces,)),
        ],
        compiler_params=pltpu.CompilerParams(
            collective_id=0, has_side_effects=True, vmem_limit_bytes=56 * 2**20
        ),
        name="expert",
    )(tokens, cotangent, routes, gate_weights, w_gate[0], w_up[0], w_down[0])

    dg, du, dd, out, dtok = pl.pallas_call(
        functools.partial(weight_kernel, own),
        out_shape=(
            jax.ShapeDtypeStruct((model, hidden), bf16),
            jax.ShapeDtypeStruct((model, hidden), bf16),
            jax.ShapeDtypeStruct((hidden, model), bf16),
            jax.ShapeDtypeStruct((own, model), bf16),
            jax.ShapeDtypeStruct((own, model), bf16),
        ),
        in_specs=[vmem] * 6,
        out_specs=(hbm,) * 3 + (vmem,) * 2,
        scratch_shapes=[
            pltpu.VMEM((model, hidden), bf16),
            pltpu.VMEM((model, hidden), bf16),
            pltpu.VMEM((hidden, model), bf16),
            pltpu.SemaphoreType.DMA((3,)),
        ],
        compiler_params=pltpu.CompilerParams(vmem_limit_bytes=60 * 2**20),
        name="weights",
    )(*(pltpu.with_memory_space_constraint(x, pltpu.VMEM) for x in (tok, cot, hid, ggp, gup, res)))

    return (out, dtok, dg[None], du[None], dd[None])


def solution(mesh):
    placed = (
        P(("ep", "tp"), None),
        P(("ep", "tp"), None),
        P(("ep", "tp"), None),
        P(("ep", "tp"), None),
        P("ep", None, "tp"),
        P("ep", None, "tp"),
        P("ep", "tp", None),
    )
    return jax.shard_map(
        functools.partial(on_device, mesh.shape["ep"], mesh.shape["tp"]),
        mesh=mesh,
        in_specs=placed,
        out_specs=(
            P(("ep", "tp"), None),
            P(("ep", "tp"), None),
            P("ep", None, "tp"),
            P("ep", None, "tp"),
            P("ep", "tp", None),
        ),
        check_vma=False,
    )
```

```python
import functools

import jax
import jax.numpy as jnp
from jax import lax
from jax.experimental import pallas as pl
from jax.experimental.pallas import tpu as pltpu
from jax.sharding import PartitionSpec as P

LANES = 128
MESH = pl.DeviceIdType.MESH


def cut(total):
    sizes = []
    for share in (2, 3):
        size = max(8, total // share // 8 * 8)
        if sum(sizes) + size < total:
            sizes.append(size)
    return sizes + [total - sum(sizes)]


def up_to(value, step):
    return -(-value // step) * step


def dot_nn(left, right):
    return lax.dot_general(left, right, (((1,), (0,)), ((), ())), preferred_element_type=jnp.float32)


def dot_nt(left, right):
    return lax.dot_general(left, right, (((1,), (1,)), ((), ())), preferred_element_type=jnp.float32)


def dot_tn(left, right):
    return lax.dot_general(left, right, (((0,), (0,)), ((), ())), preferred_element_type=jnp.float32)


def expert_kernel(
    n_ep, n_tp, n_layers, own, pad,
    tokens_hbm, cotan_hbm, routes_hbm, gates_hbm, wg_hbm, wu_hbm, wd_hbm,
    tok, cot, hid, ggp, gup, res,
    tokens_ref, cotan_ref, routes_ref, gates_ref, row32, gath, flat, wg, wu, wd, snd32, pieces,
    in_sem, w_sem, ag_send, ag_recv, fw_send, fw_recv, pr_send, pr_recv, rs_send, rs_recv,
):
    ep, tp = lax.axis_index("ep"), lax.axis_index("tp")
    side, col = lax.rem(ep, 2), ep // 2
    n_half = n_ep * n_tp // 2
    mine = col * n_tp + tp
    partner = (2 * col + 1 - side, tp)
    total, model = tok.shape
    groups = model // LANES
    n_chunks, _, width = wg.shape
    sizes = cut(2 * groups)
    n_pieces = len(sizes)
    snd, pair, half, rcv = pieces
    per = n_tp // n_layers
    spots = n_half // n_layers
    layer = tp // per
    spot = col * per + lax.rem(tp, per)

    def peer(step):
        other = lax.rem(mine + step, n_half)
        return (2 * (other // n_tp) + side, lax.rem(other, n_tp))

    inputs = [
        pltpu.make_async_copy(src, dst, in_sem.at[i])
        for i, (src, dst) in enumerate((
            (tokens_hbm, tokens_ref), (cotan_hbm, cotan_ref), (routes_hbm, routes_ref), (gates_hbm, gates_ref),
        ))
    ]
    for copy in inputs:
        copy.start()

    barrier = pltpu.get_barrier_semaphore()
    pl.semaphore_signal(barrier, inc=1, device_id=partner, device_id_type=MESH)

    @pl.loop(1, n_half)
    def _(step):
        pl.semaphore_signal(barrier, inc=1, device_id=peer(step), device_id_type=MESH)

    def weight_copies(c):
        columns = pl.ds(pl.multiple_of(c * width, width), width)
        return (
            pltpu.make_async_copy(wg_hbm.at[:, columns], wg.at[c], w_sem.at[0, c]),
            pltpu.make_async_copy(wu_hbm.at[:, columns], wu.at[c], w_sem.at[1, c]),
            pltpu.make_async_copy(wd_hbm.at[columns, :], wd.at[c], w_sem.at[2, c]),
        )

    for c in range(n_chunks):
        for copy in weight_copies(c):
            copy.start()

    row32[...] = jnp.zeros_like(row32)
    for copy in inputs:
        copy.wait()
    ids = lax.broadcasted_iota(jnp.int32, (1, LANES), 1)
    for r in range(own):
        for j in range(groups):
            lanes = slice(j * LANES, (j + 1) * LANES)
            at = r * pad + j
            row32[at:at + 1, :] = tokens_ref[r:r + 1, lanes].astype(jnp.float32)
            row32[at + groups:at + groups + 1, :] = cotan_ref[r:r + 1, lanes].astype(jnp.float32)
        gates = jnp.zeros((1, LANES), jnp.float32)
        for k in range(routes_ref.shape[1]):
            chosen = ids == routes_ref[r:r + 1, k:k + 1]
            gates = gates + jnp.where(chosen, gates_ref[r:r + 1, k:k + 1].astype(jnp.float32), 0.0)
        at = r * pad + 2 * groups
        row32[at:at + 1, :] = gates
    gath[0, layer, spot] = row32[...].astype(jnp.bfloat16)

    pl.semaphore_wait(barrier, n_half)

    low = layer < n_layers // 2
    own_block = gath.at[0, layer, spot]

    @pl.loop(0, n_half)
    def _(turn):
        its_layer = jnp.where(low, n_layers - 1 - turn // spots, turn // spots)
        its_spot = lax.rem(spot + turn, spots)

        @pl.when((its_layer != layer) | (its_spot != spot))
        def _():
            pltpu.make_async_remote_copy(
                src_ref=own_block, dst_ref=own_block,
                send_sem=ag_send.at[its_layer], recv_sem=ag_recv.at[layer],
                device_id=(2 * (its_spot // per) + side, its_layer * per + lax.rem(its_spot, per)),
                device_id_type=MESH,
            ).start()

    def await_layer(its_layer, sem):
        @pl.when(its_layer == layer)
        def _():
            rest = gath.at[0, its_layer, pl.ds(1, spots - 1)]
            pltpu.make_async_copy(rest, rest, sem.at[its_layer]).wait()

        @pl.when(its_layer != layer)
        def _():
            whole = gath.at[0, its_layer]
            pltpu.make_async_copy(whole, whole, sem.at[its_layer]).wait()

    def forward(its_layer):
        return pltpu.make_async_remote_copy(
            src_ref=gath.at[0, its_layer], dst_ref=gath.at[1, its_layer],
            send_sem=fw_send.at[its_layer], recv_sem=fw_recv.at[its_layer],
            device_id=partner, device_id_type=MESH,
        )

    block = own * pad

    def spread(which, its_side, its_layer):
        for its_spot in range(spots):
            device = (2 * (its_spot // per) + its_side) * n_tp + its_layer * per + its_spot % per
            flat[pl.ds(pl.multiple_of(device * block, 8), block), :] = (
                gath[which, its_layer, its_spot].astype(jnp.float32)
            )

    for its_layer in reversed(range(n_layers)):
        await_layer(its_layer, ag_recv)
        forward(its_layer).start()
        spread(0, side, its_layer)
    for its_layer in reversed(range(n_layers)):
        forward(its_layer).wait_recv()
        spread(1, 1 - side, its_layer)

    for j in range(groups):
        tok[:, j * LANES:(j + 1) * LANES] = flat[pl.ds(j, total, stride=pad), :].astype(jnp.bfloat16)
        cot[:, j * LANES:(j + 1) * LANES] = flat[pl.ds(groups + j, total, stride=pad), :].astype(jnp.bfloat16)
    gate_rows = flat[pl.ds(2 * groups, total, stride=pad), :]
    lane = lax.broadcasted_iota(jnp.int32, gate_rows.shape, 1)
    gate = jnp.sum(jnp.where(lane == ep, gate_rows, 0.0), axis=1, keepdims=True)

    @pl.loop(0, n_chunks)
    def _(c):
        for copy in weight_copies(c):
            copy.wait()
        gate_pre = dot_nn(tok[...], wg[c])
        up_pre = dot_nn(tok[...], wu[c])
        grad_act = dot_nt(cot[...], wd[c]) * gate
        sigmoid = jax.nn.sigmoid(gate_pre)
        silu = gate_pre * sigmoid
        columns = pl.ds(pl.multiple_of(c * width, width), width)
        hid[:, columns] = (silu * up_pre * gate).astype(jnp.bfloat16)
        ggp[:, columns] = (
            grad_act * up_pre * (sigmoid * (1.0 + gate_pre * (1.0 - sigmoid)))
        ).astype(jnp.bfloat16)
        gup[:, columns] = (grad_act * silu).astype(jnp.bfloat16)

    def pair_copy(p):
        return pltpu.make_async_remote_copy(
            src_ref=snd[p].at[1 - side], dst_ref=pair[p],
            send_sem=pr_send.at[p], recv_sem=pr_recv.at[p],
            device_id=partner, device_id_type=MESH,
        )

    def home_copies(p):
        pair_copy(p).wait_recv()
        half[p][...] = (
            snd[p][side].astype(jnp.float32) + pair[p][...].astype(jnp.float32)
        ).astype(jnp.bfloat16)

        @pl.loop(1, n_half)
        def _(step):
            pltpu.make_async_remote_copy(
                src_ref=half[p].at[lax.rem(mine + step, n_half)], dst_ref=rcv[p].at[step - 1],
                send_sem=rs_send.at[p], recv_sem=rs_recv.at[p],
                device_id=peer(step), device_id_type=MESH,
            ).start()

    unit = min(4, groups)
    for p in range(n_pieces):
        for first in range(sum(sizes[:p]), sum(sizes[:p + 1]), unit):
            start = (first % groups) * LANES
            cols = slice(start, start + unit * LANES)
            value = None
            for c in range(n_chunks):
                inner = slice(c * width, (c + 1) * width)
                if first < groups:
                    term = dot_nn(hid[:, inner], wd[c, :, cols])
                else:
                    term = dot_nt(wg[c, cols, :], ggp[:, inner]) + dot_nt(wu[c, cols, :], gup[:, inner])
                value = term if value is None else value + term
            if first >= groups:
                value = value.T
            for k in range(unit):
                snd32[pl.ds(first - sum(sizes[:p]) + k, total, stride=sizes[p]), :] = (
                    value[:, k * LANES:(k + 1) * LANES]
                )
        for d in range(2 * n_half):
            d_ep, d_tp = divmod(d, n_tp)
            snd[p][d_ep % 2, (d_ep // 2) * n_tp + d_tp] = (
                snd32[d * own * sizes[p]:(d + 1) * own * sizes[p], :].astype(jnp.bfloat16)
            )
        pair_copy(p).start()
        if p > 0:
            home_copies(p - 1)
    home_copies(n_pieces - 1)

    for p in range(n_pieces):
        pltpu.make_async_copy(rcv[p], rcv[p], rs_recv.at[p]).wait()
        res[own * sum(sizes[:p]):own * sum(sizes[:p + 1]), :] = lax.fori_loop(
            0, n_half - 1, lambda s, acc: acc + rcv[p][s].astype(jnp.float32),
            half[p][mine].astype(jnp.float32),
        )
    for its_layer in range(n_layers):
        await_layer(its_layer, ag_send)
        forward(its_layer).wait_send()
    for p in range(n_pieces):
        pair_copy(p).wait_send()
        pltpu.make_async_copy(rcv[p], rcv[p], rs_send.at[p]).wait()


def weight_kernel(own, tok, cot, hid, ggp, gup, res, dg_hbm, du_hbm, dd_hbm, out, dtok, dg, du, dd, sem):
    model, hidden = dg.shape
    tall = 192 if model % 192 == 0 else LANES
    wide = min(LANES, hidden)
    n_tall, n_wide = model // tall, hidden // wide
    done = 0
    for i in range(n_tall):
        rows = slice(i * tall, (i + 1) * tall)
        dg[rows, :] = dot_tn(tok[:, rows], ggp[...]).astype(jnp.bfloat16)
        pltpu.make_async_copy(dg.at[rows], dg_hbm.at[rows], sem.at[0]).start()
        du[rows, :] = dot_tn(tok[:, rows], gup[...]).astype(jnp.bfloat16)
        pltpu.make_async_copy(du.at[rows], du_hbm.at[rows], sem.at[1]).start()
        while done * n_tall < (i + 1) * n_wide:
            lines = slice(done * wide, (done + 1) * wide)
            dd[lines, :] = dot_tn(hid[:, lines], cot[...]).astype(jnp.bfloat16)
            pltpu.make_async_copy(dd.at[lines], dd_hbm.at[lines], sem.at[2]).start()
            done += 1

    groups = out.shape[1] // LANES
    sizes = cut(2 * groups)
    for p, size in enumerate(sizes):
        start = sum(sizes[:p])
        for r in range(own):
            for j in range(start, start + size):
                at = own * start + r * size + j - start
                k = j % groups
                ref = out if j < groups else dtok
                ref[r:r + 1, k * LANES:(k + 1) * LANES] = res[at:at + 1, :].astype(jnp.bfloat16)

    pltpu.make_async_copy(dg, dg_hbm, sem.at[0]).wait()
    pltpu.make_async_copy(du, du_hbm, sem.at[1]).wait()
    pltpu.make_async_copy(dd, dd_hbm, sem.at[2]).wait()


def on_device(n_ep, n_tp, tokens, cotangent, routes, gate_weights, w_gate, w_up, w_down):
    n = n_ep * n_tp
    own, model = tokens.shape
    hidden = w_gate.shape[2]
    total = own * n
    groups = model // LANES
    used = 2 * groups + 1
    pad = up_to(used, 8)
    width = min(256, hidden)
    n_chunks = hidden // width
    sizes = cut(2 * groups)
    n_pieces = len(sizes)

    vmem = pl.BlockSpec(memory_space=pltpu.VMEM)
    hbm = pl.BlockSpec(memory_space=pl.ANY)
    bf16 = jnp.bfloat16
    n_half = n // 2
    n_layers = 1
    while n_layers * n_layers < n_tp:
        n_layers *= 2
    tok, cot, hid, ggp, gup, res = pl.pallas_call(
        functools.partial(expert_kernel, n_ep, n_tp, n_layers, own, pad),
        out_shape=(
            pltpu.VMEM((total, model), bf16),
            pltpu.VMEM((total, model), bf16),
            pltpu.VMEM((total, hidden), bf16),
            pltpu.VMEM((total, hidden), bf16),
            pltpu.VMEM((total, hidden), bf16),
            pltpu.VMEM((own * 2 * groups, LANES), jnp.float32),
        ),
        in_specs=[hbm] * 7,
        out_specs=(vmem,) * 6,
        scratch_shapes=[
            pltpu.VMEM(tokens.shape, tokens.dtype),
            pltpu.VMEM(cotangent.shape, cotangent.dtype),
            pltpu.VMEM(routes.shape, routes.dtype),
            pltpu.VMEM(gate_weights.shape, gate_weights.dtype),
            pltpu.VMEM((own * pad, LANES), jnp.float32),
            pltpu.VMEM((2, n_layers, n_half // n_layers, own * pad, LANES), bf16),
            pltpu.VMEM((total * pad, LANES), jnp.float32),
            pltpu.VMEM((n_chunks, model, width), bf16),
            pltpu.VMEM((n_chunks, model, width), bf16),
            pltpu.VMEM((n_chunks, width, model), bf16),
            pltpu.VMEM((total * max(sizes), LANES), jnp.float32),
            tuple(
                [pltpu.VMEM((*lead, own * size, LANES), bf16) for size in sizes]
                for lead in ((2, n_half), (n_half,), (n_half,), (n_half - 1,))
            ),
            pltpu.SemaphoreType.DMA((4,)),
            pltpu.SemaphoreType.DMA((3, n_chunks)),
            pltpu.SemaphoreType.DMA((n_layers,)),
            pltpu.SemaphoreType.DMA((n_layers,)),
            pltpu.SemaphoreType.DMA((n_layers,)),
            pltpu.SemaphoreType.DMA((n_layers,)),
            pltpu.SemaphoreType.DMA((n_pieces,)),
            pltpu.SemaphoreType.DMA((n_pieces,)),
            pltpu.SemaphoreType.DMA((n_pieces,)),
            pltpu.SemaphoreType.DMA((n_pieces,)),
        ],
        compiler_params=pltpu.CompilerParams(
            collective_id=0, has_side_effects=True, vmem_limit_bytes=56 * 2**20
        ),
        name="expert",
    )(tokens, cotangent, routes, gate_weights, w_gate[0], w_up[0], w_down[0])

    dg, du, dd, out, dtok = pl.pallas_call(
        functools.partial(weight_kernel, own),
        out_shape=(
            jax.ShapeDtypeStruct((model, hidden), bf16),
            jax.ShapeDtypeStruct((model, hidden), bf16),
            jax.ShapeDtypeStruct((hidden, model), bf16),
            jax.ShapeDtypeStruct((own, model), bf16),
            jax.ShapeDtypeStruct((own, model), bf16),
        ),
        in_specs=[vmem] * 6,
        out_specs=(hbm,) * 3 + (vmem,) * 2,
        scratch_shapes=[
            pltpu.VMEM((model, hidden), bf16),
            pltpu.VMEM((model, hidden), bf16),
            pltpu.VMEM((hidden, model), bf16),
            pltpu.SemaphoreType.DMA((3,)),
        ],
        compiler_params=pltpu.CompilerParams(vmem_limit_bytes=60 * 2**20),
        name="weights",
    )(*(pltpu.with_memory_space_constraint(x, pltpu.VMEM) for x in (tok, cot, hid, ggp, gup, res)))

    return (out, dtok, dg[None], du[None], dd[None])


def solution(mesh):
    placed = (
        P(("ep", "tp"), None),
        P(("ep", "tp"), None),
        P(("ep", "tp"), None),
        P(("ep", "tp"), None),
        P("ep", None, "tp"),
        P("ep", None, "tp"),
        P("ep", "tp", None),
    )
    return jax.shard_map(
        functools.partial(on_device, mesh.shape["ep"], mesh.shape["tp"]),
        mesh=mesh,
        in_specs=placed,
        out_specs=(
            P(("ep", "tp"), None),
            P(("ep", "tp"), None),
            P("ep", None, "tp"),
            P("ep", None, "tp"),
            P("ep", "tp", None),
        ),
        check_vma=False,
    )
```

```python
import functools

import jax
import jax.numpy as jnp
from jax import lax
from jax.experimental import pallas as pl
from jax.experimental.pallas import tpu as pltpu
from jax.sharding import PartitionSpec as P

LANES = 128
MESH = pl.DeviceIdType.MESH


def cut(total):
    sizes = []
    for share in (2, 3):
        size = max(8, total // share // 8 * 8)
        if sum(sizes) + size < total:
            sizes.append(size)
    return sizes + [total - sum(sizes)]


def up_to(value, step):
    return -(-value // step) * step


def dot_nn(left, right):
    return lax.dot_general(left, right, (((1,), (0,)), ((), ())), preferred_element_type=jnp.float32)


def dot_nt(left, right):
    return lax.dot_general(left, right, (((1,), (1,)), ((), ())), preferred_element_type=jnp.float32)


def dot_tn(left, right):
    return lax.dot_general(left, right, (((0,), (0,)), ((), ())), preferred_element_type=jnp.float32)


def expert_kernel(
    n_ep, n_tp, n_layers, own, pad,
    tokens_hbm, cotan_hbm, routes_hbm, gates_hbm, wg_hbm, wu_hbm, wd_hbm,
    tok, cot, hid, ggp, gup, res,
    tokens_ref, cotan_ref, routes_ref, gates_ref, row32, gath, flat, wg, wu, wd, snd32, pieces,
    in_sem, w_sem, ag_send, ag_recv, fw_send, fw_recv, pr_send, pr_recv, rs_send, rs_recv,
):
    ep, tp = lax.axis_index("ep"), lax.axis_index("tp")
    side, col = lax.rem(ep, 2), ep // 2
    n_half = n_ep * n_tp // 2
    mine = col * n_tp + tp
    partner = (2 * col + 1 - side, tp)
    total, model = tok.shape
    groups = model // LANES
    n_chunks, _, width = wg.shape
    sizes = cut(2 * groups)
    n_pieces = len(sizes)
    snd, pair, half, rcv = pieces
    per = n_tp // n_layers
    spots = n_half // n_layers
    layer = tp // per
    spot = col * per + lax.rem(tp, per)

    def peer(step):
        other = lax.rem(mine + step, n_half)
        return (2 * (other // n_tp) + side, lax.rem(other, n_tp))

    inputs = [
        pltpu.make_async_copy(src, dst, in_sem.at[i])
        for i, (src, dst) in enumerate((
            (tokens_hbm, tokens_ref), (cotan_hbm, cotan_ref), (routes_hbm, routes_ref), (gates_hbm, gates_ref),
        ))
    ]
    for copy in inputs:
        copy.start()

    barrier = pltpu.get_barrier_semaphore()
    pl.semaphore_signal(barrier, inc=1, device_id=partner, device_id_type=MESH)

    @pl.loop(1, n_half)
    def _(step):
        pl.semaphore_signal(barrier, inc=1, device_id=peer(step), device_id_type=MESH)

    def weight_copies(c):
        columns = pl.ds(pl.multiple_of(c * width, width), width)
        return (
            pltpu.make_async_copy(wg_hbm.at[:, columns], wg.at[c], w_sem.at[0, c]),
            pltpu.make_async_copy(wu_hbm.at[:, columns], wu.at[c], w_sem.at[1, c]),
            pltpu.make_async_copy(wd_hbm.at[columns, :], wd.at[c], w_sem.at[2, c]),
        )

    for c in range(n_chunks):
        for copy in weight_copies(c):
            copy.start()

    row32[...] = jnp.zeros_like(row32)
    for copy in inputs:
        copy.wait()
    ids = lax.broadcasted_iota(jnp.int32, (1, LANES), 1)
    for r in range(own):
        for j in range(groups):
            lanes = slice(j * LANES, (j + 1) * LANES)
            at = r * pad + j
            row32[at:at + 1, :] = tokens_ref[r:r + 1, lanes].astype(jnp.float32)
            row32[at + groups:at + groups + 1, :] = cotan_ref[r:r + 1, lanes].astype(jnp.float32)
        gates = jnp.zeros((1, LANES), jnp.float32)
        for k in range(routes_ref.shape[1]):
            chosen = ids == routes_ref[r:r + 1, k:k + 1]
            gates = gates + jnp.where(chosen, gates_ref[r:r + 1, k:k + 1].astype(jnp.float32), 0.0)
        at = r * pad + 2 * groups
        row32[at:at + 1, :] = gates
    gath[0, layer, spot] = row32[...].astype(jnp.bfloat16)

    pl.semaphore_wait(barrier, n_half)

    low = layer < n_layers // 2
    own_block = gath.at[0, layer, spot]

    @pl.loop(0, n_half)
    def _(turn):
        its_layer = jnp.where(low, n_layers - 1 - turn // spots, turn // spots)
        its_spot = lax.rem(spot + turn, spots)

        @pl.when((its_layer != layer) | (its_spot != spot))
        def _():
            pltpu.make_async_remote_copy(
                src_ref=own_block, dst_ref=own_block,
                send_sem=ag_send.at[its_layer], recv_sem=ag_recv.at[layer],
                device_id=(2 * (its_spot // per) + side, its_layer * per + lax.rem(its_spot, per)),
                device_id_type=MESH,
            ).start()

    def await_layer(its_layer, sem):
        @pl.when(its_layer == layer)
        def _():
            rest = gath.at[0, its_layer, pl.ds(1, spots - 1)]
            pltpu.make_async_copy(rest, rest, sem.at[its_layer]).wait()

        @pl.when(its_layer != layer)
        def _():
            whole = gath.at[0, its_layer]
            pltpu.make_async_copy(whole, whole, sem.at[its_layer]).wait()

    def forward(its_layer):
        return pltpu.make_async_remote_copy(
            src_ref=gath.at[0, its_layer], dst_ref=gath.at[1, its_layer],
            send_sem=fw_send.at[its_layer], recv_sem=fw_recv.at[its_layer],
            device_id=partner, device_id_type=MESH,
        )

    block = own * pad

    def spread(which, its_side, its_layer):
        for its_spot in range(spots):
            device = (2 * (its_spot // per) + its_side) * n_tp + its_layer * per + its_spot % per
            flat[pl.ds(pl.multiple_of(device * block, 8), block), :] = (
                gath[which, its_layer, its_spot].astype(jnp.float32)
            )

    for its_layer in reversed(range(n_layers)):
        await_layer(its_layer, ag_recv)
        forward(its_layer).start()
        spread(0, side, its_layer)
    for its_layer in reversed(range(n_layers)):
        forward(its_layer).wait_recv()
        spread(1, 1 - side, its_layer)

    for j in range(groups):
        tok[:, j * LANES:(j + 1) * LANES] = flat[pl.ds(j, total, stride=pad), :].astype(jnp.bfloat16)
        cot[:, j * LANES:(j + 1) * LANES] = flat[pl.ds(groups + j, total, stride=pad), :].astype(jnp.bfloat16)
    gate_rows = flat[pl.ds(2 * groups, total, stride=pad), :]
    lane = lax.broadcasted_iota(jnp.int32, gate_rows.shape, 1)
    gate = jnp.sum(jnp.where(lane == ep, gate_rows, 0.0), axis=1, keepdims=True)

    @pl.loop(0, n_chunks)
    def _(c):
        for copy in weight_copies(c):
            copy.wait()
        gate_pre = dot_nn(tok[...], wg[c])
        up_pre = dot_nn(tok[...], wu[c])
        grad_act = dot_nt(cot[...], wd[c]) * gate
        sigmoid = jax.nn.sigmoid(gate_pre)
        silu = gate_pre * sigmoid
        columns = pl.ds(pl.multiple_of(c * width, width), width)
        hid[:, columns] = (silu * up_pre * gate).astype(jnp.bfloat16)
        ggp[:, columns] = (
            grad_act * up_pre * (sigmoid * (1.0 + gate_pre * (1.0 - sigmoid)))
        ).astype(jnp.bfloat16)
        gup[:, columns] = (grad_act * silu).astype(jnp.bfloat16)

    def pair_copy(p):
        return pltpu.make_async_remote_copy(
            src_ref=snd[p].at[1 - side], dst_ref=pair[p],
            send_sem=pr_send.at[p], recv_sem=pr_recv.at[p],
            device_id=partner, device_id_type=MESH,
        )

    def home_copies(p):
        pair_copy(p).wait_recv()
        half[p][...] = (
            snd[p][side].astype(jnp.float32) + pair[p][...].astype(jnp.float32)
        ).astype(jnp.bfloat16)

        @pl.loop(1, n_half)
        def _(step):
            pltpu.make_async_remote_copy(
                src_ref=half[p].at[lax.rem(mine + step, n_half)], dst_ref=rcv[p].at[step - 1],
                send_sem=rs_send.at[p], recv_sem=rs_recv.at[p],
                device_id=peer(step), device_id_type=MESH,
            ).start()

    unit = min(2, groups)
    for p in range(n_pieces):
        for first in range(sum(sizes[:p]), sum(sizes[:p + 1]), unit):
            start = (first % groups) * LANES
            cols = slice(start, start + unit * LANES)
            value = None
            for c in range(n_chunks):
                inner = slice(c * width, (c + 1) * width)
                if first < groups:
                    term = dot_nn(hid[:, inner], wd[c, :, cols])
                else:
                    term = dot_nt(wg[c, cols, :], ggp[:, inner]) + dot_nt(wu[c, cols, :], gup[:, inner])
                value = term if value is None else value + term
            if first >= groups:
                value = value.T
            for k in range(unit):
                snd32[pl.ds(first - sum(sizes[:p]) + k, total, stride=sizes[p]), :] = (
                    value[:, k * LANES:(k + 1) * LANES]
                )
        for d in range(2 * n_half):
            d_ep, d_tp = divmod(d, n_tp)
            snd[p][d_ep % 2, (d_ep // 2) * n_tp + d_tp] = (
                snd32[d * own * sizes[p]:(d + 1) * own * sizes[p], :].astype(jnp.bfloat16)
            )
        pair_copy(p).start()
        if p > 0:
            home_copies(p - 1)
    home_copies(n_pieces - 1)

    for p in range(n_pieces):
        pltpu.make_async_copy(rcv[p], rcv[p], rs_recv.at[p]).wait()
        res[own * sum(sizes[:p]):own * sum(sizes[:p + 1]), :] = lax.fori_loop(
            0, n_half - 1, lambda s, acc: acc + rcv[p][s].astype(jnp.float32),
            half[p][mine].astype(jnp.float32),
        )
    for its_layer in range(n_layers):
        await_layer(its_layer, ag_send)
        forward(its_layer).wait_send()
    for p in range(n_pieces):
        pair_copy(p).wait_send()
        pltpu.make_async_copy(rcv[p], rcv[p], rs_send.at[p]).wait()


def weight_kernel(own, tok, cot, hid, ggp, gup, res, dg_hbm, du_hbm, dd_hbm, out, dtok, dg, du, dd, sem):
    model, hidden = dg.shape
    tall = 384 if model % 384 == 0 else LANES
    wide = min(LANES, hidden)
    n_tall, n_wide = model // tall, hidden // wide
    done = 0
    for i in range(n_tall):
        rows = slice(i * tall, (i + 1) * tall)
        dg[rows, :] = dot_tn(tok[:, rows], ggp[...]).astype(jnp.bfloat16)
        pltpu.make_async_copy(dg.at[rows], dg_hbm.at[rows], sem.at[0]).start()
        du[rows, :] = dot_tn(tok[:, rows], gup[...]).astype(jnp.bfloat16)
        pltpu.make_async_copy(du.at[rows], du_hbm.at[rows], sem.at[1]).start()
        while done * n_tall < (i + 1) * n_wide:
            lines = slice(done * wide, (done + 1) * wide)
            dd[lines, :] = dot_tn(hid[:, lines], cot[...]).astype(jnp.bfloat16)
            pltpu.make_async_copy(dd.at[lines], dd_hbm.at[lines], sem.at[2]).start()
            done += 1

    groups = out.shape[1] // LANES
    sizes = cut(2 * groups)
    for p, size in enumerate(sizes):
        start = sum(sizes[:p])
        for r in range(own):
            for j in range(start, start + size):
                at = own * start + r * size + j - start
                k = j % groups
                ref = out if j < groups else dtok
                ref[r:r + 1, k * LANES:(k + 1) * LANES] = res[at:at + 1, :].astype(jnp.bfloat16)

    pltpu.make_async_copy(dg, dg_hbm, sem.at[0]).wait()
    pltpu.make_async_copy(du, du_hbm, sem.at[1]).wait()
    pltpu.make_async_copy(dd, dd_hbm, sem.at[2]).wait()


def on_device(n_ep, n_tp, tokens, cotangent, routes, gate_weights, w_gate, w_up, w_down):
    n = n_ep * n_tp
    own, model = tokens.shape
    hidden = w_gate.shape[2]
    total = own * n
    groups = model // LANES
    used = 2 * groups + 1
    pad = up_to(used, 8)
    width = min(256, hidden)
    n_chunks = hidden // width
    sizes = cut(2 * groups)
    n_pieces = len(sizes)

    vmem = pl.BlockSpec(memory_space=pltpu.VMEM)
    hbm = pl.BlockSpec(memory_space=pl.ANY)
    bf16 = jnp.bfloat16
    n_half = n // 2
    n_layers = 1
    while n_layers * n_layers < n_tp:
        n_layers *= 2
    tok, cot, hid, ggp, gup, res = pl.pallas_call(
        functools.partial(expert_kernel, n_ep, n_tp, n_layers, own, pad),
        out_shape=(
            pltpu.VMEM((total, model), bf16),
            pltpu.VMEM((total, model), bf16),
            pltpu.VMEM((total, hidden), bf16),
            pltpu.VMEM((total, hidden), bf16),
            pltpu.VMEM((total, hidden), bf16),
            pltpu.VMEM((own * 2 * groups, LANES), jnp.float32),
        ),
        in_specs=[hbm] * 7,
        out_specs=(vmem,) * 6,
        scratch_shapes=[
            pltpu.VMEM(tokens.shape, tokens.dtype),
            pltpu.VMEM(cotangent.shape, cotangent.dtype),
            pltpu.VMEM(routes.shape, routes.dtype),
            pltpu.VMEM(gate_weights.shape, gate_weights.dtype),
            pltpu.VMEM((own * pad, LANES), jnp.float32),
            pltpu.VMEM((2, n_layers, n_half // n_layers, own * pad, LANES), bf16),
            pltpu.VMEM((total * pad, LANES), jnp.float32),
            pltpu.VMEM((n_chunks, model, width), bf16),
            pltpu.VMEM((n_chunks, model, width), bf16),
            pltpu.VMEM((n_chunks, width, model), bf16),
            pltpu.VMEM((total * max(sizes), LANES), jnp.float32),
            tuple(
                [pltpu.VMEM((*lead, own * size, LANES), bf16) for size in sizes]
                for lead in ((2, n_half), (n_half,), (n_half,), (n_half - 1,))
            ),
            pltpu.SemaphoreType.DMA((4,)),
            pltpu.SemaphoreType.DMA((3, n_chunks)),
            pltpu.SemaphoreType.DMA((n_layers,)),
            pltpu.SemaphoreType.DMA((n_layers,)),
            pltpu.SemaphoreType.DMA((n_layers,)),
            pltpu.SemaphoreType.DMA((n_layers,)),
            pltpu.SemaphoreType.DMA((n_pieces,)),
            pltpu.SemaphoreType.DMA((n_pieces,)),
            pltpu.SemaphoreType.DMA((n_pieces,)),
            pltpu.SemaphoreType.DMA((n_pieces,)),
        ],
        compiler_params=pltpu.CompilerParams(
            collective_id=0, has_side_effects=True, vmem_limit_bytes=56 * 2**20
        ),
        name="expert",
    )(tokens, cotangent, routes, gate_weights, w_gate[0], w_up[0], w_down[0])

    dg, du, dd, out, dtok = pl.pallas_call(
        functools.partial(weight_kernel, own),
        out_shape=(
            jax.ShapeDtypeStruct((model, hidden), bf16),
            jax.ShapeDtypeStruct((model, hidden), bf16),
            jax.ShapeDtypeStruct((hidden, model), bf16),
            jax.ShapeDtypeStruct((own, model), bf16),
            jax.ShapeDtypeStruct((own, model), bf16),
        ),
        in_specs=[vmem] * 6,
        out_specs=(hbm,) * 3 + (vmem,) * 2,
        scratch_shapes=[
            pltpu.VMEM((model, hidden), bf16),
            pltpu.VMEM((model, hidden), bf16),
            pltpu.VMEM((hidden, model), bf16),
            pltpu.SemaphoreType.DMA((3,)),
        ],
        compiler_params=pltpu.CompilerParams(vmem_limit_bytes=60 * 2**20),
        name="weights",
    )(*(pltpu.with_memory_space_constraint(x, pltpu.VMEM) for x in (tok, cot, hid, ggp, gup, res)))

    return (out, dtok, dg[None], du[None], dd[None])


def solution(mesh):
    placed = (
        P(("ep", "tp"), None),
        P(("ep", "tp"), None),
        P(("ep", "tp"), None),
        P(("ep", "tp"), None),
        P("ep", None, "tp"),
        P("ep", None, "tp"),
        P("ep", "tp", None),
    )
    return jax.shard_map(
        functools.partial(on_device, mesh.shape["ep"], mesh.shape["tp"]),
        mesh=mesh,
        in_specs=placed,
        out_specs=(
            P(("ep", "tp"), None),
            P(("ep", "tp"), None),
            P("ep", None, "tp"),
            P("ep", None, "tp"),
            P("ep", "tp", None),
        ),
        check_vma=False,
    )
```
